32 devices in a mesh: patch: 4 (over z), seq: 4 (over y, x), req: 2 (over core).
Axes of the slice: x: 2, y: 2, z: 4, core: 2. Of those that a mesh axis runs over, the one named last changes fastest.
Arguments:
- query: bfloat16 [4, 8, 3584], P(None, ('patch', 'req')), may hold values from -20 to 20
- text_cache: bfloat16 [4, 8, 3072, 1024], P(None, ('patch', 'req'), 'seq'), may hold values from -6 to 6
- text_len: int32 [8], P(('patch', 'req')), may hold values from 0 to 3072
- image_rows: bfloat16 [4, 8192, 1024], P(None, ('patch', 'seq', 'req')), may hold values from -6 to 6
- patch_map: int32 [8192], P(('patch', 'seq', 'req')), may hold values from 0 to 7, as said below
- image_places: int32 [8192], P(('patch', 'seq', 'req')), may hold values from 0 to 1023, as said below
Outputs:
- attended: bfloat16 [4, 8, 3584], P(None, ('patch', 'req'), 'seq')
- image_cache: bfloat16 [4, 8, 1024, 1024], P(None, ('patch', 'req'), 'seq')
The draws below stay inside these ranges and needn't reach their ends.
Inputs may be any that keep to these rules, and one draw needn't show every extreme that they name: `patch_map`: each aligned block of 256 rows (the rows of one prefill device) holds exactly 32 rows of every request. `image_places`: together with patch_map every pair of request and position occurs exactly once. The rows of a device whose seq index is s have positions from s * 256 to (s + 1) * 256 - 1.
All inputs are finite; a program needn't handle non-finite values.
Results may differ from the reference program's by a relative error of at most 0.0026.
Values may be sent and summed in bfloat16 or wider, within the bound.
A program may use at most 64 MiB of HBM per device.

```python
import math
import jax
import jax.numpy as jnp
from jax import lax

HEADS = 28
KV_HEADS = 4
HEAD_DIM = 128
LAYERS = 4
IMG = 1024
TXT = 3072
REQUESTS = 8
KVW = 512
N_PATCH = 4
N_SEQ = 4
N_REQ = 2


def layout_rows(key):
    groups = N_PATCH * N_REQ
    band_size = IMG // N_SEQ
    per_source = band_size // groups
    device_count = N_PATCH * N_SEQ * N_REQ
    pair_keys = jax.random.split(jax.random.fold_in(key, 7001), N_SEQ * REQUESTS)
    shuffled = jax.vmap(lambda piece: jax.random.permutation(piece, band_size))(pair_keys)
    shuffled = shuffled.astype(jnp.int32).reshape(N_SEQ, REQUESTS, N_PATCH, N_REQ, per_source)
    band_start = (jnp.arange(N_SEQ, dtype=jnp.int32) * band_size)[:, None, None, None, None]
    places = shuffled + band_start
    owners = jnp.broadcast_to(jnp.arange(REQUESTS, dtype=jnp.int32)[None, :, None, None, None], places.shape)
    places = jnp.transpose(places, (2, 0, 3, 1, 4)).reshape(device_count, REQUESTS * per_source)
    owners = jnp.transpose(owners, (2, 0, 3, 1, 4)).reshape(device_count, REQUESTS * per_source)
    row_keys = jax.random.split(jax.random.fold_in(key, 7002), device_count)
    mixing = jax.vmap(lambda piece: jax.random.permutation(piece, REQUESTS * per_source))(row_keys)
    mixing = mixing.astype(jnp.int32)
    places = jnp.take_along_axis(places, mixing, axis=1).reshape(-1)
    owners = jnp.take_along_axis(owners, mixing, axis=1).reshape(-1)
    return (owners, places)


def draw_patch_map(key, part):
    return layout_rows(key)[0]


def draw_image_places(key, part):
    return layout_rows(key)[1]


def draw_query(key, part):
    shape = (LAYERS, REQUESTS, HEADS * HEAD_DIM)
    noise_key = jax.random.fold_in(key, 7004)
    values = jnp.clip(2.5 * jax.random.normal(noise_key, shape, jnp.float32), -12.0, 12.0)
    return values.astype(jnp.bfloat16)


def draw_image_rows(key, part):
    shape = (LAYERS, REQUESTS * IMG, 2 * KV_HEADS * HEAD_DIM)
    noise_key = jax.random.fold_in(key, 7005)
    values = jnp.clip(jax.random.normal(noise_key, shape, jnp.float32), -6.0, 6.0)
    return values.astype(jnp.bfloat16)


def place_ends(values, own_key, least, top_value):
    index_at = [jax.random.randint(jax.random.fold_in(own_key, axis), (), 0, length) for axis, length in enumerate(values.shape)]
    longest = values.shape.index(max(values.shape))
    neighbour = index_at[:longest] + [(index_at[longest] + 1) % values.shape[longest]] + index_at[longest + 1:]
    return values.at[tuple(index_at)].set(least).at[tuple(neighbour)].set(top_value)


def block_levels(rng, shape, cuts, low, largest):
    loudness, own = 1.0, jax.random.fold_in(rng, 6)
    for position, shards_of in cuts:
        steps = jnp.exp(jax.random.uniform(jax.random.fold_in(own, position), (shards_of,), jnp.float32, low / len(cuts), largest / len(cuts)))
        loudness = loudness * jnp.repeat(steps, shape[position] // shards_of).reshape([-1 if axis == position else 1 for axis in range(len(shape))])
    return loudness


def bell_draw(rng, dims, deviation, most, cuts=(), kind=jnp.bfloat16):
    result = deviation * jax.random.normal(rng, dims, jnp.float32)
    if cuts:
        result = result * block_levels(rng, dims, cuts, -0.22, 0.18)
    return jnp.clip(result, -most, most).astype(kind)


def setup_inputs(seed: int = 0) -> dict:
    seeds = jax.random.split(jax.random.key(seed), 7)
    return {
        "query": draw_query(jax.random.fold_in(seeds[6], 71), 0),
        "text_cache": bell_draw(seeds[1], (LAYERS, REQUESTS, TXT, 2 * KVW), 1.0, 6.0, ((1, 8), (2, 4))),
        "text_len": place_ends(jax.random.randint(seeds[2], (REQUESTS,), 0, TXT + 1), jax.random.fold_in(seeds[2], 1), 0, TXT).astype(jnp.int32),
        "image_rows": draw_image_rows(jax.random.fold_in(seeds[6], 71), 0),
        "patch_map": draw_patch_map(jax.random.fold_in(seeds[6], 71), 0),
        "image_places": draw_image_places(jax.random.fold_in(seeds[6], 71), 0),
    }


def attend_one(query_row, image_block, text_block, length):
    kv_width = KV_HEADS * HEAD_DIM
    group = HEADS // KV_HEADS
    band_size = IMG // N_SEQ
    text_band = TXT // N_SEQ
    image_banded = image_block.reshape(N_SEQ, band_size, 2 * kv_width)
    text_banded = text_block.reshape(N_SEQ, text_band, 2 * kv_width)
    keys_all = jnp.concatenate([image_banded, text_banded], axis=1)
    width = band_size + text_band
    keys = keys_all[:, :, :kv_width].reshape(N_SEQ, width, KV_HEADS, HEAD_DIM).astype(jnp.float32)
    values = keys_all[:, :, kv_width:].reshape(N_SEQ, width, KV_HEADS, HEAD_DIM).astype(jnp.float32)
    queries = query_row.reshape(KV_HEADS, group, HEAD_DIM).astype(jnp.float32)
    scores = jnp.einsum('kgd,stkd->skgt', queries, keys) * (1.0 / math.sqrt(HEAD_DIM))
    inner = jnp.arange(width, dtype=jnp.int32)
    bands = jnp.arange(N_SEQ, dtype=jnp.int32)
    text_pos = bands[:, None] * text_band + inner[None, :] - band_size
    used = (inner[None, :] < band_size) | (text_pos < length)
    scores = jnp.where(used[:, None, None, :], scores, -jnp.inf)
    band_top = lax.optimization_barrier(jnp.max(scores, axis=-1, keepdims=True))
    weights = jnp.exp(scores - band_top)
    band_total = lax.optimization_barrier(jnp.sum(weights, axis=-1))
    rounded = lax.optimization_barrier(weights.astype(jnp.bfloat16)).astype(jnp.float32)
    band_sum = jnp.einsum('skgt,stkd->skgd', rounded, values)
    band_top = band_top[..., 0]
    top = lax.optimization_barrier(jnp.max(band_top, axis=0, keepdims=True))
    factor = jnp.exp(band_top - top)
    total = lax.optimization_barrier(jnp.sum(factor * band_total, axis=0))
    summed = lax.optimization_barrier(jnp.sum(factor[..., None] * band_sum, axis=0))
    return (summed / total[..., None]).reshape(HEADS * HEAD_DIM).astype(jnp.bfloat16)

def attend_packed(packed):
    return attend_one(packed[0], packed[1], packed[2], packed[3])

def reference(query, text_cache, text_len, image_rows, patch_map, image_places):
    order = jnp.argsort(patch_map * IMG + image_places)
    image_cache = jnp.take(image_rows, order, axis=1).reshape(LAYERS, REQUESTS, IMG, image_rows.shape[2])

    def per_layer(packed):
        return lax.map(attend_packed, (packed[0], packed[1], packed[2], text_len))
    attended = lax.map(per_layer, (query, image_cache, text_cache))
    return (attended, image_cache)
```

```python
import functools
import math

import jax
import jax.numpy as jnp
from jax import lax
from jax.experimental import pallas as pl
from jax.experimental.pallas import tpu as pltpu
from jax.sharding import PartitionSpec as P

HEADS = 28
KV_HEADS = 4
HEAD_DIM = 128
PAD = 8
MESH = pl.DeviceIdType.MESH
NT = (((1,), (1,)), ((), ()))


def hop_order(patch_count, req_count):
    steps = sorted(range(1, patch_count), key=lambda d: -min(d, patch_count - d))
    pairs = [(d, c) for d in steps for c in range(req_count)]
    return pairs + [(0, c) for c in range(1, req_count)]


def kernel(
    dims,
    query_ref, len_ref, map_ref, place_ref, rows_hbm, text_hbm,
    att_ref, cache_hbm,
    rows, text, grouped, arrived, cache, place_out, place_in, scores, part_out, part_in,
    rows_sem, text_sem, cache_sem, img_send, img_recv, place_send, place_recv,
    part_send, part_recv,
):
    patch_count, seq_count, req_count = dims
    layers, src_rows, full = rows.shape
    text_dev = text.shape[1]
    kvw = full // 2
    group = HEADS // KV_HEADS
    groups = patch_count * req_count
    per = src_rows // groups
    scale = 1.0 / math.sqrt(HEAD_DIM)
    patch, seq, req = (lax.axis_index(a) for a in ("patch", "seq", "req"))
    me = patch * req_count + req
    hops = hop_order(patch_count, req_count)

    for l in range(layers):
        pltpu.make_async_copy(rows_hbm.at[l], rows.at[l], rows_sem.at[l]).start()
    for l in range(layers):
        pltpu.make_async_copy(text_hbm.at[l, 0], text.at[l], text_sem.at[l]).start()

    def partner(hop):
        p = lax.rem(patch + hop[0], patch_count)
        r = lax.rem(req + hop[1], req_count)
        return p, r

    barrier = pltpu.get_barrier_semaphore()
    for hop in hops:
        p, r = partner(hop)
        pl.semaphore_signal(barrier, inc=1, device_id=(p, seq, r), device_id_type=MESH)
    for d in range(1, seq_count):
        s = lax.rem(seq + d, seq_count)
        pl.semaphore_signal(barrier, inc=1, device_id=(patch, s, req), device_id_type=MESH)

    f32, bf16 = jnp.float32, jnp.bfloat16
    owner = lax.broadcasted_iota(jnp.int32, (groups, src_rows), 0)
    mine = map_ref[...] == owner
    row_i = lax.broadcasted_iota(jnp.int32, (src_rows, src_rows), 0)
    col_i = lax.broadcasted_iota(jnp.int32, (src_rows, src_rows), 1)
    before = (row_i < col_i).astype(f32).astype(bf16)
    rank = jnp.dot(mine.astype(f32).astype(bf16), before, preferred_element_type=f32)
    slot = jnp.sum(
        jnp.where(mine, rank + (owner * per).astype(f32), 0.0), axis=0, keepdims=True
    )
    pick = (row_i == slot.astype(jnp.int32)).astype(f32).astype(bf16)
    local = (place_ref[...] - seq * src_rows).astype(f32).astype(bf16)
    place_sorted = lax.dot_general(
        jnp.broadcast_to(local, (PAD, src_rows)), pick, NT, preferred_element_type=f32
    )
    place_out[...] = place_sorted[0:1].astype(jnp.int32)
    place_in[me] = place_sorted[0:1].astype(jnp.int32)

    pl.semaphore_wait(barrier, len(hops) + seq_count - 1)

    def place_copy(k, hop):
        p, r = partner(hop)
        return pltpu.make_async_remote_copy(
            src_ref=place_out, dst_ref=place_in.at[me],
            send_sem=place_send.at[k], recv_sem=place_recv.at[k],
            device_id=(p, seq, r), device_id_type=MESH,
        )

    def image_copy(l, k, hop):
        p, r = partner(hop)
        return pltpu.make_async_remote_copy(
            src_ref=grouped.at[l, p * req_count + r], dst_ref=arrived.at[l, me],
            send_sem=img_send.at[l, k], recv_sem=img_recv.at[l, k],
            device_id=(p, seq, r), device_id_type=MESH,
        )

    def part_copy(l, d):
        s = lax.rem(seq + d, seq_count)
        return pltpu.make_async_remote_copy(
            src_ref=part_out.at[l, s], dst_ref=part_in.at[l, d],
            send_sem=part_send.at[l, d], recv_sem=part_recv.at[l, d],
            device_id=(patch, s, req), device_id_type=MESH,
        )

    for l in range(layers):
        pltpu.make_async_copy(rows_hbm.at[l], rows.at[l], rows_sem.at[l]).wait()
        moved = jnp.dot(pick, rows[l], preferred_element_type=f32).astype(bf16)
        grouped[l] = moved.reshape(groups, per, full)
        if l == 0:
            for k, hop in enumerate(hops):
                place_copy(k, hop).start()
        for k, hop in enumerate(hops):
            image_copy(l, k, hop).start()
    for l in range(layers):
        arrived[l, me] = grouped[l, me]

    positions = seq * text_dev + lax.broadcasted_iota(
        jnp.int32, (KV_HEADS * PAD, text_dev), 1
    )
    used = positions < len_ref[0]
    zeros = jnp.zeros((PAD, HEAD_DIM), bf16)
    spread = []
    for l in range(layers):
        line = query_ref[l].astype(f32)
        blocks = []
        for g in range(KV_HEADS):
            heads = [
                line[:, (g * group + h) * HEAD_DIM:(g * group + h + 1) * HEAD_DIM]
                for h in range(group)
            ] + [jnp.zeros((PAD - group, HEAD_DIM), f32)]
            block = jnp.concatenate(heads, axis=0).astype(bf16)
            blocks.append(
                jnp.concatenate(
                    [block if c == g else zeros for c in range(KV_HEADS)], axis=1
                )
            )
        spread.append(jnp.concatenate(blocks, axis=0))
    for l in range(layers):
        pltpu.make_async_copy(text_hbm.at[l, 0], text.at[l], text_sem.at[l]).wait()
        raw = lax.dot_general(
            spread[l], text[l, :, :kvw], NT, preferred_element_type=f32
        ) * scale
        scores[l] = jnp.where(used, raw, -jnp.inf)

    for k, hop in enumerate(hops):
        place_copy(k, hop).wait_recv()
    wanted = (row_i == me * per + lax.rem(col_i, per)).astype(f32).astype(bf16)
    lanes = jnp.dot(
        place_in[...].reshape(groups, src_rows).astype(f32).astype(bf16), wanted,
        preferred_element_type=f32,
    )
    source = lax.broadcasted_iota(jnp.int32, (groups, src_rows), 1) // per
    place = jnp.sum(jnp.where(source == owner, lanes, 0.0), axis=0, keepdims=True)
    put = (row_i == place.astype(jnp.int32)).astype(f32).astype(bf16)

    for l in range(layers):
        for k, hop in enumerate(hops):
            image_copy(l, k, hop).wait_recv()
        block = arrived[l].reshape(src_rows, full)
        image_scores = lax.dot_general(
            spread[l], block[:, :kvw], NT, preferred_element_type=f32
        ) * scale
        text_scores = scores[l]
        top = jnp.maximum(
            jnp.max(text_scores, axis=1, keepdims=True),
            jnp.max(image_scores, axis=1, keepdims=True),
        )
        text_w = jnp.exp(text_scores - top)
        image_w = jnp.exp(image_scores - top)
        total = jnp.sum(text_w, axis=1, keepdims=True) + jnp.sum(
            image_w, axis=1, keepdims=True
        )
        values = jnp.dot(
            image_w.astype(bf16), block[:, kvw:], preferred_element_type=f32
        ) + jnp.dot(text_w.astype(bf16), text[l, :, kvw:], preferred_element_type=f32)
        for g in range(KV_HEADS):
            at = slice(g * PAD, (g + 1) * PAD)
            cell = jnp.concatenate(
                [
                    values[at, g * HEAD_DIM:(g + 1) * HEAD_DIM],
                    jnp.broadcast_to(top[at], (PAD, HEAD_DIM)),
                    jnp.broadcast_to(total[at], (PAD, HEAD_DIM)),
                ],
                axis=1,
            )
            part_out[l, g] = cell
        for d in range(1, seq_count):
            part_copy(l, d).start()
        cache[l] = jnp.dot(put, block, preferred_element_type=f32).astype(bf16)
        pltpu.make_async_copy(cache.at[l], cache_hbm.at[l, 0], cache_sem.at[l]).start()

    for l in range(layers):
        for d in range(1, seq_count):
            part_copy(l, d).wait_recv()
        cells = [part_out[l, seq]] + [part_in[l, d] for d in range(1, seq_count)]
        tops = [c[:, HEAD_DIM:2 * HEAD_DIM] for c in cells]
        top = functools.reduce(jnp.maximum, tops)
        factors = [jnp.exp(t - top) for t in tops]
        total = sum(f * c[:, 2 * HEAD_DIM:] for f, c in zip(factors, cells))
        summed = sum(f * c[:, :HEAD_DIM] for f, c in zip(factors, cells))
        result = summed / total
        att_ref[l] = jnp.concatenate(
            [result[h:h + 1] for h in range(group)], axis=1
        ).astype(bf16)

    for l in range(layers):
        pltpu.make_async_copy(cache.at[l], cache_hbm.at[l, 0], cache_sem.at[l]).wait()
        for k, hop in enumerate(hops):
            image_copy(l, k, hop).wait_send()
        for d in range(1, seq_count):
            part_copy(l, d).wait_send()
    for k, hop in enumerate(hops):
        place_copy(k, hop).wait_send()


def body(dims, query, text_cache, text_len, image_rows, patch_map, image_places):
    patch_count, seq_count, req_count = dims
    layers, req_dev, query_width = query.shape
    text_dev, full = text_cache.shape[2:]
    src_rows = image_rows.shape[1]
    groups = patch_count * req_count
    assert req_dev == 1 and seq_count == KV_HEADS and full == 2 * KV_HEADS * HEAD_DIM
    per = src_rows // groups
    hops = groups - 1
    bf16, f32 = jnp.bfloat16, jnp.float32
    dma = pltpu.SemaphoreType.DMA
    vmem = pl.BlockSpec(memory_space=pltpu.VMEM)
    hbm = pl.BlockSpec(memory_space=pl.ANY)
    return pl.pallas_call(
        functools.partial(kernel, dims),
        out_shape=(
            jax.ShapeDtypeStruct((layers, 1, query_width // seq_count), bf16),
            jax.ShapeDtypeStruct((layers, 1, src_rows, full), bf16),
        ),
        in_specs=[vmem, pl.BlockSpec(memory_space=pltpu.SMEM), vmem, vmem, hbm, hbm],
        out_specs=(vmem, hbm),
        scratch_shapes=[
            pltpu.VMEM((layers, src_rows, full), bf16),
            pltpu.VMEM((layers, text_dev, full), bf16),
            pltpu.VMEM((layers, groups, per, full), bf16),
            pltpu.VMEM((layers, groups, per, full), bf16),
            pltpu.VMEM((layers, src_rows, full), bf16),
            pltpu.VMEM((1, src_rows), jnp.int32),
            pltpu.VMEM((groups, 1, src_rows), jnp.int32),
            pltpu.VMEM((layers, KV_HEADS * PAD, text_dev), f32),
            pltpu.VMEM((layers, KV_HEADS, PAD, 3 * HEAD_DIM), f32),
            pltpu.VMEM((layers, seq_count, PAD, 3 * HEAD_DIM), f32),
            dma((layers,)), dma((layers,)), dma((layers,)),
            dma((layers, hops)), dma((layers, hops)), dma((hops,)), dma((hops,)),
            dma((layers, seq_count)), dma((layers, seq_count)),
        ],
        compiler_params=pltpu.CompilerParams(
            collective_id=0, has_side_effects=True, vmem_limit_bytes=48 * 1024 * 1024
        ),
    )(
        query, text_len, patch_map.reshape(1, src_rows), image_places.reshape(1, src_rows),
        image_rows, text_cache,
    )


def solution(mesh):
    dims = tuple(mesh.shape[a] for a in ("patch", "seq", "req"))
    return jax.shard_map(
        functools.partial(body, dims),
        mesh=mesh,
        in_specs=(
            P(None, ("patch", "req"), None),
            P(None, ("patch", "req"), "seq", None),
            P(("patch", "req")),
            P(None, ("patch", "seq", "req"), None),
            P(("patch", "seq", "req")),
            P(("patch", "seq", "req")),
        ),
        out_specs=(P(None, ("patch", "req"), "seq"), P(None, ("patch", "req"), "seq", None)),
        check_vma=False,
    )
```

```python
import functools
import math

import jax
import jax.numpy as jnp
from jax import lax
from jax.experimental import pallas as pl
from jax.experimental.pallas import tpu as pltpu
from jax.sharding import PartitionSpec as P

HEADS = 28
KV_HEADS = 4
HEAD_DIM = 128
PAD = 8
MESH = pl.DeviceIdType.MESH
NT = (((1,), (1,)), ((), ()))


def hop_order(patch_count, req_count):
    steps = sorted(range(1, patch_count), key=lambda d: -min(d, patch_count - d))
    pairs = [(d, c) for d in steps for c in range(req_count)]
    return pairs + [(0, c) for c in range(1, req_count)]


def kernel(
    dims,
    query_ref, len_ref, map_hbm, place_hbm, rows_hbm, text_hbm,
    att_ref, cache,
    query, maps, places, rows, text, main_out, main_in, own_out, own_in, place_out, place_in,
    scores, image_ws, text_sums, image_sums, part_out, part_in,
    small_sem, rows_sem, text_sem, main_send, main_recv, own_send, own_recv,
    place_send, place_recv, part_send, part_recv,
):
    patch_count, seq_count, req_count = dims
    layers, src_rows, full = rows.shape
    text_dev = text.shape[1]
    kvw = full // 2
    group = HEADS // KV_HEADS
    groups = patch_count * req_count
    per = src_rows // groups
    main_width = full - HEAD_DIM
    scale = 1.0 / math.sqrt(HEAD_DIM)
    patch, seq, req = (lax.axis_index(a) for a in ("patch", "seq", "req"))
    me = patch * req_count + req
    hops = hop_order(patch_count, req_count)
    f32, bf16 = jnp.float32, jnp.bfloat16

    small = [
        pltpu.make_async_copy(map_hbm, maps, small_sem.at[0]),
        pltpu.make_async_copy(place_hbm, places, small_sem.at[1]),
        pltpu.make_async_copy(query_ref, query, small_sem.at[2]),
    ]
    for copy in small:
        copy.start()

    def rows_copy(l):
        return pltpu.make_async_copy(rows_hbm.at[l], rows.at[l], rows_sem.at[l])

    def text_copy(l):
        return pltpu.make_async_copy(text_hbm.at[l, 0], text.at[l], text_sem.at[l])

    for l in range(layers):
        rows_copy(l).start()
    for l in range(layers):
        text_copy(l).start()

    def partner(hop):
        p = lax.rem(patch + hop[0], patch_count)
        r = lax.rem(req + hop[1], req_count)
        return p, r

    def lanes_of(d):
        g = lax.rem(seq + d, seq_count)
        return pl.ds(pl.multiple_of(kvw + g * HEAD_DIM, HEAD_DIM), HEAD_DIM)

    barrier = pltpu.get_barrier_semaphore()
    for hop in hops:
        p, r = partner(hop)
        pl.semaphore_signal(barrier, inc=1, device_id=(p, seq, r), device_id_type=MESH)
    for d in range(1, seq_count):
        s = lax.rem(seq + d, seq_count)
        pl.semaphore_signal(barrier, inc=1, device_id=(patch, s, req), device_id_type=MESH)

    owner = lax.broadcasted_iota(jnp.int32, (groups, src_rows), 0)
    row_i = lax.broadcasted_iota(jnp.int32, (src_rows, src_rows), 0)
    col_i = lax.broadcasted_iota(jnp.int32, (src_rows, src_rows), 1)
    before = (row_i < col_i).astype(f32).astype(bf16)
    small[0].wait()
    mine = maps[...] == owner
    rank = jnp.dot(mine.astype(f32).astype(bf16), before, preferred_element_type=f32)
    slot = jnp.sum(
        jnp.where(mine, rank + (owner * per).astype(f32), 0.0), axis=0, keepdims=True
    )
    pick = (row_i == slot.astype(jnp.int32)).astype(f32).astype(bf16)

    def place_copy(k, hop):
        p, r = partner(hop)
        return pltpu.make_async_remote_copy(
            src_ref=place_out, dst_ref=place_in.at[me],
            send_sem=place_send.at[k], recv_sem=place_recv.at[k],
            device_id=(p, seq, r), device_id_type=MESH,
        )

    def main_copy(l, k, hop):
        p, r = partner(hop)
        return pltpu.make_async_remote_copy(
            src_ref=main_out.at[l, p * req_count + r], dst_ref=main_in.at[l, me],
            send_sem=main_send.at[l, k], recv_sem=main_recv.at[l, k],
            device_id=(p, seq, r), device_id_type=MESH,
        )

    def own_copy(k, hop):
        p, r = partner(hop)
        return pltpu.make_async_remote_copy(
            src_ref=own_out.at[p * req_count + r], dst_ref=own_in.at[me],
            send_sem=own_send.at[k], recv_sem=own_recv.at[k],
            device_id=(p, seq, r), device_id_type=MESH,
        )

    def part_copy(l, d):
        s = lax.rem(seq + d, seq_count)
        return pltpu.make_async_remote_copy(
            src_ref=part_out.at[l, d], dst_ref=part_in.at[l, d],
            send_sem=part_send.at[l, d], recv_sem=part_recv.at[l, d],
            device_id=(patch, s, req), device_id_type=MESH,
        )

    for l in range(layers):
        rows_copy(l).wait()
        keys = jnp.dot(pick, rows[l, :, :kvw], preferred_element_type=f32).astype(bf16)
        main_out[l, :, :, :kvw] = keys.reshape(groups, per, kvw)
        others = jnp.concatenate(
            [rows[l, :, lanes_of(d)] for d in range(1, seq_count)] + [rows[l, :, lanes_of(0)]],
            axis=1,
        )
        moved = jnp.dot(pick, others, preferred_element_type=f32).astype(bf16)
        cut = main_width - kvw
        main_out[l, :, :, kvw:] = moved[:, :cut].reshape(groups, per, cut)
        own_out[:, l] = moved[:, cut:].reshape(groups, per, HEAD_DIM)
        if l == 0:
            pl.semaphore_wait(barrier, len(hops) + seq_count - 1)
        for k, hop in enumerate(hops):
            main_copy(l, k, hop).start()
        if l == 0:
            small[1].wait()
            local = (places[...] - seq * src_rows).astype(f32).astype(bf16)
            place_sorted = lax.dot_general(
                jnp.broadcast_to(local, (PAD, src_rows)), pick, NT,
                preferred_element_type=f32,
            )
            place_out[...] = place_sorted[0:1].astype(jnp.int32)
            place_in[me] = place_sorted[0:1].astype(jnp.int32)
            for k, hop in enumerate(hops):
                place_copy(k, hop).start()
    for k, hop in enumerate(hops):
        own_copy(k, hop).start()
    for l in range(layers):
        main_in[l, me] = main_out[l, me]
    own_in[me] = own_out[me]

    positions = seq * text_dev + lax.broadcasted_iota(
        jnp.int32, (KV_HEADS * PAD, text_dev), 1
    )
    used = positions < len_ref[0]
    zeros = jnp.zeros((PAD, HEAD_DIM), bf16)
    small[2].wait()
    lines = query[...].astype(f32)
    spread = []
    for l in range(layers):
        blocks = []
        for g in range(KV_HEADS):
            heads = [
                lines[l:l + 1, (g * group + h) * HEAD_DIM:(g * group + h + 1) * HEAD_DIM]
                for h in range(group)
            ] + [jnp.zeros((PAD - group, HEAD_DIM), f32)]
            block = jnp.concatenate(heads, axis=0).astype(bf16)
            blocks.append(
                jnp.concatenate(
                    [block if c == g else zeros for c in range(KV_HEADS)], axis=1
                )
            )
        spread.append(jnp.concatenate(blocks, axis=0))
    for l in range(layers):
        text_copy(l).wait()
        raw = lax.dot_general(
            spread[l], text[l, :, :kvw], NT, preferred_element_type=f32
        ) * scale
        scores[l] = jnp.where(used, raw, -jnp.inf)

    for k, hop in enumerate(hops):
        place_copy(k, hop).wait_recv()
    wanted = (row_i == me * per + lax.rem(col_i, per)).astype(f32).astype(bf16)
    lanes = jnp.dot(
        place_in[...].reshape(groups, src_rows).astype(f32).astype(bf16), wanted,
        preferred_element_type=f32,
    )
    source = lax.broadcasted_iota(jnp.int32, (groups, src_rows), 1) // per
    place = jnp.sum(jnp.where(source == owner, lanes, 0.0), axis=0, keepdims=True)
    put = (row_i == place.astype(jnp.int32)).astype(f32).astype(bf16)

    for l in range(layers):
        for k, hop in enumerate(hops):
            main_copy(l, k, hop).wait_recv()
        block = main_in[l].reshape(src_rows, main_width)
        image_scores = lax.dot_general(
            spread[l], block[:, :kvw], NT, preferred_element_type=f32
        ) * scale
        text_scores = scores[l]
        top = jnp.maximum(
            jnp.max(text_scores, axis=1, keepdims=True),
            jnp.max(image_scores, axis=1, keepdims=True),
        )
        text_w = jnp.exp(text_scores - top)
        image_w = jnp.exp(image_scores - top)
        total = jnp.sum(text_w, axis=1, keepdims=True) + jnp.sum(
            image_w, axis=1, keepdims=True
        )
        text_sums[:, :kvw] = jnp.dot(
            text_w.astype(bf16), text[l, :, kvw:], preferred_element_type=f32
        )
        text_sums[:, kvw:kvw + HEAD_DIM] = jnp.broadcast_to(top, (KV_HEADS * PAD, HEAD_DIM))
        text_sums[:, kvw + HEAD_DIM:] = jnp.broadcast_to(total, (KV_HEADS * PAD, HEAD_DIM))
        image_sums[...] = jnp.dot(
            image_w.astype(bf16), block[:, kvw:], preferred_element_type=f32
        )
        image_ws[l] = image_w
        for d in range(seq_count):
            g = lax.rem(seq + d, seq_count)
            at = pl.ds(pl.multiple_of(g * PAD, PAD), PAD)
            value = text_sums[at, pl.ds(pl.multiple_of(g * HEAD_DIM, HEAD_DIM), HEAD_DIM)]
            if d:
                value = value + image_sums[at, (d - 1) * HEAD_DIM:d * HEAD_DIM]
            part_out[l, d, :, :HEAD_DIM] = value
            part_out[l, d, :, HEAD_DIM:] = text_sums[at, kvw:]
            if d:
                part_copy(l, d).start()
        moved = jnp.dot(put, block, preferred_element_type=f32).astype(bf16)
        cache[l, 0, :, :kvw] = moved[:, :kvw]
        for d in range(1, seq_count):
            cache[l, 0, :, lanes_of(d)] = moved[
                :, kvw + (d - 1) * HEAD_DIM:kvw + d * HEAD_DIM
            ]

    partial = []
    for l in range(layers):
        for d in range(1, seq_count):
            part_copy(l, d).wait_recv()
        cells = [part_out[l, 0]] + [part_in[l, d] for d in range(1, seq_count)]
        tops = [c[:, HEAD_DIM:2 * HEAD_DIM] for c in cells]
        top = functools.reduce(jnp.maximum, tops)
        factors = [jnp.exp(t - top) for t in tops]
        total = sum(f * c[:, 2 * HEAD_DIM:] for f, c in zip(factors, cells))
        summed = sum(f * c[:, :HEAD_DIM] for f, c in zip(factors, cells))
        partial.append((factors[0], summed, total))

    for k, hop in enumerate(hops):
        own_copy(k, hop).wait_recv()
    at = pl.ds(pl.multiple_of(seq * PAD, PAD), PAD)
    own_values = [own_in[:, l].reshape(src_rows, HEAD_DIM) for l in range(layers)]
    lines = []
    for l in range(layers):
        factor, summed, total = partial[l]
        value = jnp.dot(
            image_ws[l, at, :].astype(bf16), own_values[l], preferred_element_type=f32
        )
        result = (summed + factor * value) / total
        lines.append(jnp.concatenate([result[h:h + 1] for h in range(group)], axis=1))
    att_ref[...] = jnp.concatenate(lines, axis=0).astype(bf16)
    moved = jnp.dot(
        put, jnp.concatenate(own_values, axis=1), preferred_element_type=f32
    ).astype(bf16)
    for l in range(layers):
        cache[l, 0, :, lanes_of(0)] = moved[:, l * HEAD_DIM:(l + 1) * HEAD_DIM]

    for l in range(layers):
        for k, hop in enumerate(hops):
            main_copy(l, k, hop).wait_send()
        for d in range(1, seq_count):
            part_copy(l, d).wait_send()
    for k, hop in enumerate(hops):
        own_copy(k, hop).wait_send()
        place_copy(k, hop).wait_send()


def finish(att_ref, cache_ref, att_out, cache_out, sem):
    layers = cache_ref.shape[0]
    copies = [
        pltpu.make_async_copy(cache_ref.at[l], cache_out.at[l], sem.at[l])
        for l in range(layers)
    ]
    for copy in copies:
        copy.start()
    att_out[...] = att_ref[...]
    for copy in copies:
        copy.wait()


def body(dims, query, text_cache, text_len, image_rows, patch_map, image_places):
    patch_count, seq_count, req_count = dims
    layers, req_dev, query_width = query.shape
    text_dev, full = text_cache.shape[2:]
    src_rows = image_rows.shape[1]
    groups = patch_count * req_count
    assert req_dev == 1 and seq_count == KV_HEADS and full == 2 * KV_HEADS * HEAD_DIM
    per = src_rows // groups
    hops = groups - 1
    kvw = full // 2
    main_width = full - HEAD_DIM
    rows_padded = KV_HEADS * PAD
    bf16, f32, i32 = jnp.bfloat16, jnp.float32, jnp.int32
    dma = pltpu.SemaphoreType.DMA
    vmem = pl.BlockSpec(memory_space=pltpu.VMEM)
    hbm = pl.BlockSpec(memory_space=pltpu.HBM)
    att_shape = jax.ShapeDtypeStruct((layers, query_width // seq_count), bf16)
    cache_shape = jax.ShapeDtypeStruct((layers, 1, src_rows, full), bf16)
    in_hbm = lambda x: pltpu.with_memory_space_constraint(x, pltpu.HBM)
    in_vmem = lambda x: pltpu.with_memory_space_constraint(x, pltpu.VMEM)
    attended, cache = pl.pallas_call(
        functools.partial(kernel, dims),
        out_shape=(
            pltpu.VMEM(att_shape.shape, bf16), pltpu.VMEM(cache_shape.shape, bf16)
        ),
        in_specs=[hbm, pl.BlockSpec(memory_space=pltpu.SMEM), hbm, hbm, hbm, hbm],
        out_specs=(vmem, vmem),
        scratch_shapes=[
            pltpu.VMEM((layers, query_width), bf16),
            pltpu.VMEM((1, src_rows), i32),
            pltpu.VMEM((1, src_rows), i32),
            pltpu.VMEM((layers, src_rows, full), bf16),
            pltpu.VMEM((layers, text_dev, full), bf16),
            pltpu.VMEM((layers, groups, per, main_width), bf16),
            pltpu.VMEM((layers, groups, per, main_width), bf16),
            pltpu.VMEM((groups, layers, per, HEAD_DIM), bf16),
            pltpu.VMEM((groups, layers, per, HEAD_DIM), bf16),
            pltpu.VMEM((1, src_rows), i32),
            pltpu.VMEM((groups, 1, src_rows), i32),
            pltpu.VMEM((layers, rows_padded, text_dev), f32),
            pltpu.VMEM((layers, rows_padded, src_rows), f32),
            pltpu.VMEM((rows_padded, kvw + 2 * HEAD_DIM), f32),
            pltpu.VMEM((rows_padded, main_width - kvw), f32),
            pltpu.VMEM((layers, seq_count, PAD, 3 * HEAD_DIM), f32),
            pltpu.VMEM((layers, seq_count, PAD, 3 * HEAD_DIM), f32),
            dma((3,)), dma((layers,)), dma((layers,)),
            dma((layers, hops)), dma((layers, hops)), dma((hops,)), dma((hops,)),
            dma((hops,)), dma((hops,)), dma((layers, seq_count)), dma((layers, seq_count)),
        ],
        compiler_params=pltpu.CompilerParams(
            collective_id=0, has_side_effects=True, vmem_limit_bytes=32 * 1024 * 1024
        ),
    )(
        in_hbm(query.reshape(layers, query_width)), text_len,
        in_hbm(patch_map.reshape(1, src_rows)), in_hbm(image_places.reshape(1, src_rows)),
        in_hbm(image_rows), in_hbm(text_cache),
    )
    attended, cache = pl.pallas_call(
        finish,
        out_shape=(att_shape, cache_shape),
        in_specs=[vmem, vmem],
        out_specs=(vmem, hbm),
        scratch_shapes=[dma((layers,))],
    )(in_vmem(attended), in_vmem(cache))
    return attended.reshape(layers, 1, query_width // seq_count), cache


def solution(mesh):
    dims = tuple(mesh.shape[a] for a in ("patch", "seq", "req"))
    return jax.shard_map(
        functools.partial(body, dims),
        mesh=mesh,
        in_specs=(
            P(None, ("patch", "req"), None),
            P(None, ("patch", "req"), "seq", None),
            P(("patch", "req")),
            P(None, ("patch", "seq", "req"), None),
            P(("patch", "seq", "req")),
            P(("patch", "seq", "req")),
        ),
        out_specs=(P(None, ("patch", "req"), "seq"), P(None, ("patch", "req"), "seq", None)),
        check_vma=False,
    )
```

```python
import functools
import math

import jax
import jax.numpy as jnp
from jax import lax
from jax.experimental import pallas as pl
from jax.experimental.pallas import tpu as pltpu
from jax.sharding import PartitionSpec as P

HEADS = 28
KV_HEADS = 4
HEAD_DIM = 128
PAD = 8
MESH = pl.DeviceIdType.MESH
NT = (((1,), (1,)), ((), ()))


def hop_order(patch_count, req_count):
    steps = sorted(range(1, patch_count), key=lambda d: -min(d, patch_count - d))
    pairs = [(d, c) for d in steps for c in range(req_count)]
    return pairs + [(0, c) for c in range(1, req_count)]


def kernel(
    dims,
    query_ref, len_hbm, map_hbm, place_hbm, rows_hbm, text_hbm,
    att_ref, cache,
    query, length, maps, places, rows, text, main_out, main_in, own_out, own_in, place_out, place_in,
    scores, image_ws, text_sums, image_sums, part_out, part_in,
    small_sem, rows_sem, text_sem, main_send, main_recv, own_send, own_recv,
    place_send, place_recv, part_send, part_recv,
):
    patch_count, seq_count, req_count = dims
    layers, src_rows, full = rows.shape
    text_dev = text.shape[1]
    kvw = full // 2
    group = HEADS // KV_HEADS
    groups = patch_count * req_count
    per = src_rows // groups
    main_width = full - HEAD_DIM
    scale = 1.0 / math.sqrt(HEAD_DIM)
    patch, seq, req = (lax.axis_index(a) for a in ("patch", "seq", "req"))
    me = patch * req_count + req
    hops = hop_order(patch_count, req_count)
    f32, bf16 = jnp.float32, jnp.bfloat16

    def partner(hop):
        p = lax.rem(patch + hop[0], patch_count)
        r = lax.rem(req + hop[1], req_count)
        return p, r

    barrier = pltpu.get_barrier_semaphore()
    for hop in hops:
        p, r = partner(hop)
        pl.semaphore_signal(barrier, inc=1, device_id=(p, seq, r), device_id_type=MESH)
    for d in range(1, seq_count):
        s = lax.rem(seq + d, seq_count)
        pl.semaphore_signal(barrier, inc=1, device_id=(patch, s, req), device_id_type=MESH)

    small = [
        pltpu.make_async_copy(map_hbm, maps, small_sem.at[0]),
        pltpu.make_async_copy(place_hbm, places, small_sem.at[1]),
        pltpu.make_async_copy(query_ref, query, small_sem.at[2]),
        pltpu.make_async_copy(len_hbm, length, small_sem.at[3]),
    ]
    for copy in small:
        copy.start()

    def rows_copy(l):
        return pltpu.make_async_copy(rows_hbm.at[l], rows.at[l], rows_sem.at[l])

    def text_copy(l):
        return pltpu.make_async_copy(text_hbm.at[l, 0], text.at[l], text_sem.at[l])

    rows_copy(0).start()

    def lanes_of(d):
        g = lax.rem(seq + d, seq_count)
        return pl.ds(pl.multiple_of(kvw + g * HEAD_DIM, HEAD_DIM), HEAD_DIM)

    owner = lax.broadcasted_iota(jnp.int32, (groups, src_rows), 0)
    row_i = lax.broadcasted_iota(jnp.int32, (src_rows, src_rows), 0)
    col_i = lax.broadcasted_iota(jnp.int32, (src_rows, src_rows), 1)
    before = (row_i < col_i).astype(f32).astype(bf16)
    small[0].wait()
    mine = maps[...] == owner
    rank = jnp.dot(mine.astype(f32).astype(bf16), before, preferred_element_type=f32)
    slot = jnp.sum(
        jnp.where(mine, rank + (owner * per).astype(f32), 0.0), axis=0, keepdims=True
    )
    pick = (row_i == slot.astype(jnp.int32)).astype(f32).astype(bf16)

    def place_copy(k, hop):
        p, r = partner(hop)
        return pltpu.make_async_remote_copy(
            src_ref=place_out, dst_ref=place_in.at[me],
            send_sem=place_send.at[k], recv_sem=place_recv.at[k],
            device_id=(p, seq, r), device_id_type=MESH,
        )

    def main_copy(l, k, hop):
        p, r = partner(hop)
        return pltpu.make_async_remote_copy(
            src_ref=main_out.at[l, p * req_count + r], dst_ref=main_in.at[l, me],
            send_sem=main_send.at[l, k], recv_sem=main_recv.at[l, k],
            device_id=(p, seq, r), device_id_type=MESH,
        )

    def own_copy(k, hop):
        p, r = partner(hop)
        return pltpu.make_async_remote_copy(
            src_ref=own_out.at[p * req_count + r], dst_ref=own_in.at[me],
            send_sem=own_send.at[k], recv_sem=own_recv.at[k],
            device_id=(p, seq, r), device_id_type=MESH,
        )

    def part_copy(l, d):
        s = lax.rem(seq + d, seq_count)
        return pltpu.make_async_remote_copy(
            src_ref=part_out.at[l, d], dst_ref=part_in.at[l, d],
            send_sem=part_send.at[l, d], recv_sem=part_recv.at[l, d],
            device_id=(patch, s, req), device_id_type=MESH,
        )

    for l in range(layers):
        rows_copy(l).wait()
        if l == 0:
            for m in range(1, layers):
                rows_copy(m).start()
        keys = jnp.dot(pick, rows[l, :, :kvw], preferred_element_type=f32).astype(bf16)
        main_out[l, :, :, :kvw] = keys.reshape(groups, per, kvw)
        others = jnp.concatenate(
            [rows[l, :, lanes_of(d)] for d in range(1, seq_count)] + [rows[l, :, lanes_of(0)]],
            axis=1,
        )
        moved = jnp.dot(pick, others, preferred_element_type=f32).astype(bf16)
        cut = main_width - kvw
        main_out[l, :, :, kvw:] = moved[:, :cut].reshape(groups, per, cut)
        own_out[:, l] = moved[:, cut:].reshape(groups, per, HEAD_DIM)
        if l == 0:
            pl.semaphore_wait(barrier, len(hops) + seq_count - 1)
        for k, hop in enumerate(hops):
            main_copy(l, k, hop).start()
        if l == 0:
            small[1].wait()
            local = (places[...] - seq * src_rows).astype(f32).astype(bf16)
            place_sorted = lax.dot_general(
                jnp.broadcast_to(local, (PAD, src_rows)), pick, NT,
                preferred_element_type=f32,
            )
            place_out[...] = place_sorted[0:1].astype(jnp.int32)
            place_in[me] = place_sorted[0:1].astype(jnp.int32)
            for k, hop in enumerate(hops):
                place_copy(k, hop).start()
    for k, hop in enumerate(hops):
        own_copy(k, hop).start()
    for l in range(layers):
        text_copy(l).start()
    for l in range(layers):
        main_in[l, me] = main_out[l, me]
    own_in[me] = own_out[me]

    positions = seq * text_dev + lax.broadcasted_iota(
        jnp.int32, (KV_HEADS * PAD, text_dev), 1
    )
    small[3].wait()
    used = positions < length[0:1, 0:1]
    zeros = jnp.zeros((PAD, HEAD_DIM), bf16)
    small[2].wait()
    lines = query[...].astype(f32)
    spread = []
    for l in range(layers):
        blocks = []
        for g in range(KV_HEADS):
            heads = [
                lines[l:l + 1, (g * group + h) * HEAD_DIM:(g * group + h + 1) * HEAD_DIM]
                for h in range(group)
            ] + [jnp.zeros((PAD - group, HEAD_DIM), f32)]
            block = jnp.concatenate(heads, axis=0).astype(bf16)
            blocks.append(
                jnp.concatenate(
                    [block if c == g else zeros for c in range(KV_HEADS)], axis=1
                )
            )
        spread.append(jnp.concatenate(blocks, axis=0))
    for l in range(layers):
        text_copy(l).wait()
        raw = lax.dot_general(
            spread[l], text[l, :, :kvw], NT, preferred_element_type=f32
        ) * scale
        scores[l] = jnp.where(used, raw, -jnp.inf)

    for k, hop in enumerate(hops):
        place_copy(k, hop).wait_recv()
    wanted = (row_i == me * per + lax.rem(col_i, per)).astype(f32).astype(bf16)
    lanes = jnp.dot(
        place_in[...].reshape(groups, src_rows).astype(f32).astype(bf16), wanted,
        preferred_element_type=f32,
    )
    source = lax.broadcasted_iota(jnp.int32, (groups, src_rows), 1) // per
    place = jnp.sum(jnp.where(source == owner, lanes, 0.0), axis=0, keepdims=True)
    put = (row_i == place.astype(jnp.int32)).astype(f32).astype(bf16)

    for l in range(layers):
        for k, hop in enumerate(hops):
            main_copy(l, k, hop).wait_recv()
        block = main_in[l].reshape(src_rows, main_width)
        image_scores = lax.dot_general(
            spread[l], block[:, :kvw], NT, preferred_element_type=f32
        ) * scale
        text_scores = scores[l]
        top = jnp.maximum(
            jnp.max(text_scores, axis=1, keepdims=True),
            jnp.max(image_scores, axis=1, keepdims=True),
        )
        text_w = jnp.exp(text_scores - top)
        image_w = jnp.exp(image_scores - top)
        total = jnp.sum(text_w, axis=1, keepdims=True) + jnp.sum(
            image_w, axis=1, keepdims=True
        )
        text_sums[:, :kvw] = jnp.dot(
            text_w.astype(bf16), text[l, :, kvw:], preferred_element_type=f32
        )
        text_sums[:, kvw:kvw + HEAD_DIM] = jnp.broadcast_to(top, (KV_HEADS * PAD, HEAD_DIM))
        text_sums[:, kvw + HEAD_DIM:] = jnp.broadcast_to(total, (KV_HEADS * PAD, HEAD_DIM))
        image_sums[...] = jnp.dot(
            image_w.astype(bf16), block[:, kvw:], preferred_element_type=f32
        )
        image_ws[l] = image_w
        for d in range(seq_count):
            g = lax.rem(seq + d, seq_count)
            at = pl.ds(pl.multiple_of(g * PAD, PAD), PAD)
            value = text_sums[at, pl.ds(pl.multiple_of(g * HEAD_DIM, HEAD_DIM), HEAD_DIM)]
            if d:
                value = value + image_sums[at, (d - 1) * HEAD_DIM:d * HEAD_DIM]
            part_out[l, d, :, :HEAD_DIM] = value
            part_out[l, d, :, HEAD_DIM:] = text_sums[at, kvw:]
            if d:
                part_copy(l, d).start()
        moved = jnp.dot(put, block, preferred_element_type=f32).astype(bf16)
        cache[l, 0, :, :kvw] = moved[:, :kvw]
        for d in range(1, seq_count):
            cache[l, 0, :, lanes_of(d)] = moved[
                :, kvw + (d - 1) * HEAD_DIM:kvw + d * HEAD_DIM
            ]

    partial = []
    for l in range(layers):
        for d in range(1, seq_count):
            part_copy(l, d).wait_recv()
        cells = [part_out[l, 0]] + [part_in[l, d] for d in range(1, seq_count)]
        tops = [c[:, HEAD_DIM:2 * HEAD_DIM] for c in cells]
        top = functools.reduce(jnp.maximum, tops)
        factors = [jnp.exp(t - top) for t in tops]
        total = sum(f * c[:, 2 * HEAD_DIM:] for f, c in zip(factors, cells))
        summed = sum(f * c[:, :HEAD_DIM] for f, c in zip(factors, cells))
        partial.append((factors[0], summed, total))

    for k, hop in enumerate(hops):
        own_copy(k, hop).wait_recv()
    at = pl.ds(pl.multiple_of(seq * PAD, PAD), PAD)
    own_values = [own_in[:, l].reshape(src_rows, HEAD_DIM) for l in range(layers)]
    lines = []
    for l in range(layers):
        factor, summed, total = partial[l]
        value = jnp.dot(
            image_ws[l, at, :].astype(bf16), own_values[l], preferred_element_type=f32
        )
        result = (summed + factor * value) / total
        lines.append(jnp.concatenate([result[h:h + 1] for h in range(group)], axis=1))
    att_ref[...] = jnp.concatenate(lines, axis=0).astype(bf16)
    moved = jnp.dot(
        put, jnp.concatenate(own_values, axis=1), preferred_element_type=f32
    ).astype(bf16)
    for l in range(layers):
        cache[l, 0, :, lanes_of(0)] = moved[:, l * HEAD_DIM:(l + 1) * HEAD_DIM]

    for l in range(layers):
        for k, hop in enumerate(hops):
            main_copy(l, k, hop).wait_send()
        for d in range(1, seq_count):
            part_copy(l, d).wait_send()
    for k, hop in enumerate(hops):
        own_copy(k, hop).wait_send()
        place_copy(k, hop).wait_send()


def finish(att_ref, cache_ref, att_out, cache_out, sem, small_sem):
    layers, pieces = sem.shape
    step = cache_ref.shape[2] // pieces
    copies = [
        pltpu.make_async_copy(
            cache_ref.at[l, :, i * step:(i + 1) * step],
            cache_out.at[l, :, i * step:(i + 1) * step],
            sem.at[l, i],
        )
        for l in range(layers)
        for i in range(pieces)
    ]
    copies.append(pltpu.make_async_copy(att_ref, att_out, small_sem.at[0]))
    for copy in copies:
        copy.start()
    for copy in copies:
        copy.wait()


def body(dims, query, text_cache, text_len, image_rows, patch_map, image_places):
    patch_count, seq_count, req_count = dims
    layers, req_dev, query_width = query.shape
    text_dev, full = text_cache.shape[2:]
    src_rows = image_rows.shape[1]
    groups = patch_count * req_count
    assert req_dev == 1 and seq_count == KV_HEADS and full == 2 * KV_HEADS * HEAD_DIM
    per = src_rows // groups
    hops = groups - 1
    kvw = full // 2
    main_width = full - HEAD_DIM
    rows_padded = KV_HEADS * PAD
    bf16, f32, i32 = jnp.bfloat16, jnp.float32, jnp.int32
    dma = pltpu.SemaphoreType.DMA
    vmem = pl.BlockSpec(memory_space=pltpu.VMEM)
    hbm = pl.BlockSpec(memory_space=pltpu.HBM)
    att_shape = jax.ShapeDtypeStruct((layers, query_width // seq_count), bf16)
    cache_shape = jax.ShapeDtypeStruct((layers, 1, src_rows, full), bf16)
    in_hbm = lambda x: pltpu.with_memory_space_constraint(x, pltpu.HBM)
    in_vmem = lambda x: pltpu.with_memory_space_constraint(x, pltpu.VMEM)
    attended, cache = pl.pallas_call(
        functools.partial(kernel, dims),
        out_shape=(
            pltpu.VMEM(att_shape.shape, bf16), pltpu.VMEM(cache_shape.shape, bf16)
        ),
        in_specs=[hbm, pl.BlockSpec(memory_space=pl.ANY), hbm, hbm, hbm, hbm],
        out_specs=(vmem, vmem),
        scratch_shapes=[
            pltpu.VMEM((layers, query_width), bf16),
            pltpu.VMEM((PAD, HEAD_DIM), i32),
            pltpu.VMEM((1, src_rows), i32),
            pltpu.VMEM((1, src_rows), i32),
            pltpu.VMEM((layers, src_rows, full), bf16),
            pltpu.VMEM((layers, text_dev, full), bf16),
            pltpu.VMEM((layers, groups, per, main_width), bf16),
            pltpu.VMEM((layers, groups, per, main_width), bf16),
            pltpu.VMEM((groups, layers, per, HEAD_DIM), bf16),
            pltpu.VMEM((groups, layers, per, HEAD_DIM), bf16),
            pltpu.VMEM((1, src_rows), i32),
            pltpu.VMEM((groups, 1, src_rows), i32),
            pltpu.VMEM((layers, rows_padded, text_dev), f32),
            pltpu.VMEM((layers, rows_padded, src_rows), f32),
            pltpu.VMEM((rows_padded, kvw + 2 * HEAD_DIM), f32),
            pltpu.VMEM((rows_padded, main_width - kvw), f32),
            pltpu.VMEM((layers, seq_count, PAD, 3 * HEAD_DIM), f32),
            pltpu.VMEM((layers, seq_count, PAD, 3 * HEAD_DIM), f32),
            dma((4,)), dma((layers,)), dma((layers,)),
            dma((layers, hops)), dma((layers, hops)), dma((hops,)), dma((hops,)),
            dma((hops,)), dma((hops,)), dma((layers, seq_count)), dma((layers, seq_count)),
        ],
        compiler_params=pltpu.CompilerParams(
            collective_id=0, has_side_effects=True, vmem_limit_bytes=32 * 1024 * 1024
        ),
    )(
        in_hbm(query.reshape(layers, query_width)), jnp.broadcast_to(text_len.reshape(1, 1), (PAD, HEAD_DIM)),
        in_hbm(patch_map.reshape(1, src_rows)), in_hbm(image_places.reshape(1, src_rows)),
        in_hbm(image_rows), in_hbm(text_cache),
    )
    attended, cache = pl.pallas_call(
        finish,
        out_shape=(att_shape, cache_shape),
        in_specs=[vmem, vmem],
        out_specs=(hbm, hbm),
        scratch_shapes=[dma((layers, 4)), dma((1,))],
    )(in_vmem(attended), in_vmem(cache))
    return attended.reshape(layers, 1, query_width // seq_count), cache


def solution(mesh):
    dims = tuple(mesh.shape[a] for a in ("patch", "seq", "req"))
    return jax.shard_map(
        functools.partial(body, dims),
        mesh=mesh,
        in_specs=(
            P(None, ("patch", "req"), None),
            P(None, ("patch", "req"), "seq", None),
            P(("patch", "req")),
            P(None, ("patch", "seq", "req"), None),
            P(("patch", "seq", "req")),
            P(("patch", "seq", "req")),
        ),
        out_specs=(P(None, ("patch", "req"), "seq"), P(None, ("patch", "req"), "seq", None)),
        check_vma=False,
    )
```
